16 devices in a mesh: dp: 2 (over y, z), sp: 8 (over x, core).
Axes of the slice: x: 4, y: 2, z: 1, core: 2. Of those that a mesh axis runs over, the one named last changes fastest.
The devices are a block of a 4x4x8 slice.
Arguments:
- q: bfloat16 [64, 8, 256], P('dp'), parts along dimension 0
- k: bfloat16 [64, 4096, 8, 256], P('dp', 'sp'), parts along dimension 0
- v: bfloat16 [64, 4096, 8, 256], P('dp', 'sp'), parts along dimension 0
Outputs:
- q: bfloat16 [64, 8, 256], P('dp'), parts along dimension 0
There are 2 independent parts. The reference program is written for one: setup_inputs(seed, part) draws one part's arguments, and reference() takes and returns one part's arrays. A program takes and returns all parts, laid end to end along the dimension named above; each array names one.
All inputs are finite; a program needn't handle non-finite values.
Results may differ from the reference program's by a relative error of at most 0.012.
Values are sent between devices in bfloat16 or wider.
A program may use at most 768 MiB of HBM per device.

```python
import jax
import jax.numpy as jnp

BATCH = 32
CACHE = 4096
HEADS = 8
KV_HEADS = 8
HEAD = 256


def setup_inputs(seed: int = 0, part: int = 0) -> dict:
    kq, kk, kv = (jax.random.fold_in(k, part) for k in jax.random.split(jax.random.key(seed), 3))
    return {
        "q": (3 * jax.random.normal(kq, (BATCH, HEADS, HEAD), jnp.float32)).astype(jnp.bfloat16),
        "k": jax.random.normal(kk, (BATCH, CACHE, KV_HEADS, HEAD), jnp.float32).astype(jnp.bfloat16),
        "v": jax.random.normal(kv, (BATCH, CACHE, KV_HEADS, HEAD), jnp.float32).astype(jnp.bfloat16),
    }


def einsum(form, a, b):
    return jnp.einsum(form, a.astype(jnp.float32), b.astype(jnp.float32))


def reference(q, k, v):
    grouped = q.reshape(BATCH, KV_HEADS, -1, HEAD)
    scores = einsum("bgsd,bugd->bgsu", grouped, k) * HEAD**-0.5
    weights = jax.nn.softmax(scores, -1).astype(jnp.bfloat16)
    return einsum("bgsu,bugd->bgsd", weights, v).astype(jnp.bfloat16).reshape(BATCH, HEADS, HEAD)
```

```python
import functools

import jax
import jax.numpy as jnp
from jax import lax
from jax.experimental import pallas as pl
from jax.experimental.pallas import tpu as pltpu
from jax.sharding import PartitionSpec as P

SLOTS = 4
GROUP = 2
MESH = pl.DeviceIdType.MESH


def iotas():
    return lax.broadcasted_iota(jnp.int32, (8, 128), 1), lax.broadcasted_iota(jnp.int32, (8, 128), 0)


def scores_of(q, k_ref):
    lane, sub = iotas()
    spread = jnp.concatenate([q] * 16, 0)
    full = lax.dot_general(k_ref[...], spread, (((1,), (1,)), ((), ())), preferred_element_type=jnp.float32)
    full = full.reshape(-1, 16, 8, 128)
    out = []
    for r in range(full.shape[0]):
        level = [full[r, i] for i in range(16)]
        bit = 8
        while len(level) > 1:
            level = [jnp.where((lane & bit) != 0, level[i + 1], level[i]) for i in range(0, len(level), 2)]
            bit *= 2
        out.append(jnp.sum(jnp.where((lane & 7) == sub, level[0], 0.0), 0, keepdims=True))
    return jnp.concatenate(out, 0)


def fold(x, op):
    turned = [x] + [pltpu.roll(x, s, 1) for s in range(8, 128, 8)]
    while len(turned) > 1:
        turned = [op(turned[i], turned[i + 1]) for i in range(0, len(turned), 2)]
    return turned[0]


def kernel(q_ref, k_ref, v_ref, o_ref, k_buf, v_buf, gathered, sums, k_sem, v_sem, send_sem, recv_sem, send_sum, recv_sum):
    batch = k_ref.shape[0]
    n = lax.axis_size("sp")
    me = lax.axis_index("sp")
    lane, sub = iotas()
    diag = (lane & 7) == sub

    def k_copy(b, slot):
        return pltpu.make_async_copy(k_ref.at[b], k_buf.at[slot], k_sem.at[slot])

    def v_copy(b, slot):
        return pltpu.make_async_copy(v_ref.at[b], v_buf.at[slot], v_sem.at[slot])

    k_copy(0, 0).start()
    k_copy(1, 1).start()
    for b in range(2, SLOTS):
        v_copy(b - 2, b - 2).start()
        k_copy(b, b).start()
    v_copy(SLOTS - 2, SLOTS - 2).start()
    v_copy(SLOTS - 1, SLOTS - 1).start()

    barrier = pltpu.get_barrier_semaphore()
    for step in range(1, n):
        pl.semaphore_signal(barrier, inc=1, device_id={"sp": lax.rem(me + step, n)}, device_id_type=MESH)

    def score(b, slot):
        return scores_of(q_ref[b], k_buf.at[slot]) * k_ref.shape[2] ** -0.5

    def soften(s):
        high = fold(jnp.max(s, 0, keepdims=True), jnp.maximum)
        p = jnp.exp(s - high)
        total = fold(jnp.sum(p, 0, keepdims=True), jnp.add)
        return p, jnp.where(lane[:1] < 64, high, total)

    def weigh(p, slot):
        big = [jnp.where(diag, jnp.broadcast_to(p[r:r + 1], (8, 128)), 0.0) for r in range(p.shape[0])]
        return jnp.dot(jnp.concatenate(big, 1).astype(jnp.bfloat16), v_buf[slot], preferred_element_type=jnp.float32)

    def copies(first, count, which, owner, step):
        peer = {"sp": lax.rem(me + step, n)}
        block, block_sums = gathered.at[owner, pl.ds(first, count)], sums.at[owner, pl.ds(first, count)]
        return (
            pltpu.make_async_remote_copy(block, block, send_sem.at[which, step], recv_sem.at[which, owner], device_id=peer, device_id_type=MESH),
            pltpu.make_async_remote_copy(block_sums, block_sums, send_sum.at[which, step], recv_sum.at[which, owner], device_id=peer, device_id_type=MESH),
        )

    def send(first, count, which):
        for step in range(1, n):
            for copy in copies(first, count, which, me, step):
                copy.start()

    def received(first, count, which):
        for step in range(1, n):
            for copy in copies(first, count, which, lax.rem(me + step, n), step):
                copy.wait_recv()

    def sent(first, count, which):
        for step in range(1, n):
            for copy in copies(first, count, which, me, step):
                copy.wait_send()

    def combine(b):
        rows = jnp.concatenate([sums[d, b] for d in range(n)], 0)
        high = jnp.max(rows, 0, keepdims=True)
        scale = jnp.exp(rows - high)
        total = jnp.sum(pltpu.roll(rows, 64, 1) * scale, 0, keepdims=True)
        scale = scale / total
        result = jnp.zeros(o_ref.shape[1:], jnp.float32)
        for d in range(n):
            column = jnp.sum(jnp.where(lane == sub, jnp.broadcast_to(scale[d:d + 1], (8, 128)), 0.0), 1, keepdims=True)
            result += gathered[d, b].astype(jnp.float32) * column
        o_ref[b] = result.astype(o_ref.dtype)

    main = batch - 2

    k_copy(0, 0).wait()
    s0 = score(0, 0)
    k_copy(1, 1).wait()
    p0, row = soften(s0)
    s1 = score(1, 1)
    sums[me, 0] = row
    for b in range(2):
        k_copy(b + SLOTS, b).start()
    pl.semaphore_wait(barrier, n - 1)

    def body(b, carry):
        s, p = carry
        slot, k_slot = lax.rem(b, SLOTS), lax.rem(b + 2, SLOTS)
        v_copy(b, slot).wait()
        k_copy(b + 2, k_slot).wait()
        gathered[me, b] = weigh(p, slot).astype(jnp.bfloat16)
        s_next = score(b + 2, k_slot)
        p_next, row = soften(s)
        sums[me, b + 1] = row

        @pl.when(b + SLOTS < batch)
        def _():
            v_copy(b + SLOTS, slot).start()

        @pl.when(b + 2 + SLOTS < batch)
        def _():
            k_copy(b + 2 + SLOTS, k_slot).start()

        @pl.when(lax.rem(b, GROUP) == GROUP - 1)
        def _():
            send(b - (GROUP - 1), GROUP, 0)

        return s_next, p_next

    s, p = lax.fori_loop(0, batch - 2, body, (s1, p0))
    v_copy(main, main % SLOTS).wait()
    gathered[me, main] = weigh(p, main % SLOTS).astype(jnp.bfloat16)
    p, row = soften(s)
    last = batch - 1
    sums[me, last] = row
    send(main, 1, 1)
    v_copy(last, last % SLOTS).wait()
    gathered[me, last] = weigh(p, last % SLOTS).astype(jnp.bfloat16)
    send(last, 1, 2)

    received(0, main, 0)

    def finish(i, _):
        for j in range(5):
            combine(i * 5 + j)
        return 0

    lax.fori_loop(0, main // 5, finish, 0)
    received(main, 1, 1)
    combine(main)
    received(last, 1, 2)
    combine(last)
    sent(0, main, 0)
    sent(main, 1, 1)
    sent(last, 1, 2)


def solution(mesh):
    n = mesh.shape["sp"]

    def step(q, k, v):
        b, u, h, d = k.shape
        rows = u * h
        return pl.pallas_call(
            kernel,
            out_shape=jax.ShapeDtypeStruct((b, h, d), jnp.bfloat16),
            in_specs=[pl.BlockSpec(memory_space=pltpu.VMEM), pl.BlockSpec(memory_space=pl.ANY), pl.BlockSpec(memory_space=pl.ANY)],
            out_specs=pl.BlockSpec(memory_space=pltpu.VMEM),
            scratch_shapes=[
                pltpu.VMEM((SLOTS, rows, d), jnp.bfloat16),
                pltpu.VMEM((SLOTS, rows, d), jnp.bfloat16),
                pltpu.VMEM((n, b, h, d), jnp.bfloat16),
                pltpu.VMEM((n, b, 1, 128), jnp.float32),
                pltpu.SemaphoreType.DMA((SLOTS,)),
                pltpu.SemaphoreType.DMA((SLOTS,)),
                pltpu.SemaphoreType.DMA((3, n)),
                pltpu.SemaphoreType.DMA((3, n)),
                pltpu.SemaphoreType.DMA((3, n)),
                pltpu.SemaphoreType.DMA((3, n)),
            ],
            name="decode",
            compiler_params=pltpu.CompilerParams(collective_id=0, has_side_effects=True, vmem_limit_bytes=60 * 1024 * 1024),
        )(q, k.reshape(b, rows, d), v.reshape(b, rows, d))

    return jax.shard_map(
        step,
        mesh=mesh,
        in_specs=(P("dp", None, None), P("dp", "sp", None, None), P("dp", "sp", None, None)),
        out_specs=P("dp", None, None),
        check_vma=False,
    )
```

```python
import functools

import jax
import jax.numpy as jnp
from jax import lax
from jax.experimental import pallas as pl
from jax.experimental.pallas import tpu as pltpu
from jax.sharding import PartitionSpec as P

SLOTS = 4
FLIGHT = 2 * (SLOTS - 1)
GROUP = 2
PIECES = 4
LIMIT = 32
MESH = pl.DeviceIdType.MESH


def iotas():
    return lax.broadcasted_iota(jnp.int32, (8, 128), 1), lax.broadcasted_iota(jnp.int32, (8, 128), 0)


def scores_of(q, k_ref):
    lane, sub = iotas()
    spread = jnp.concatenate([q] * 16, 0)
    full = lax.dot_general(k_ref[...], spread, (((1,), (1,)), ((), ())), preferred_element_type=jnp.float32)
    full = full.reshape(-1, 16, 8, 128)
    out = []
    for r in range(full.shape[0]):
        level = [full[r, i] for i in range(16)]
        bit = 8
        while len(level) > 1:
            level = [jnp.where((lane & bit) != 0, level[i + 1], level[i]) for i in range(0, len(level), 2)]
            bit *= 2
        out.append(jnp.sum(jnp.where((lane & 7) == sub, level[0], 0.0), 0, keepdims=True))
    return jnp.concatenate(out, 0)


def fold(x, op):
    turned = [x] + [pltpu.roll(x, s, 1) for s in range(8, 128, 8)]
    while len(turned) > 1:
        turned = [op(turned[i], turned[i + 1]) for i in range(0, len(turned), 2)]
    return turned[0]


def kernel(q_hbm, k_ref, v_ref, o_ref, q_ref, k_buf, v_buf, gathered, sums, q_sem, k_sem, v_sem, last_sem, send_sem, recv_sem, send_sum, recv_sum):
    batch = k_ref.shape[0]
    n = lax.axis_size("sp")
    me = lax.axis_index("sp")
    lane, sub = iotas()
    diag = (lane & 7) == sub

    def k_copy(b, slot):
        return pltpu.make_async_copy(k_ref.at[b], k_buf.at[slot], k_sem.at[slot])

    def last_copy(piece):
        rows = v_ref.shape[1] // PIECES
        part = pl.ds(piece * rows, rows)
        return pltpu.make_async_copy(v_ref.at[batch - 1, part], v_buf.at[(batch - 1) % SLOTS, part], last_sem.at[piece])

    def v_copy(b, slot):
        return pltpu.make_async_copy(v_ref.at[b], v_buf.at[slot], v_sem.at[slot])

    q_copy = pltpu.make_async_copy(q_hbm, q_ref, q_sem)
    def start(i):
        if i == 0 or i % 2:
            b = 0 if i == 0 else (i + 1) // 2
            k_copy(b, b % SLOTS).start()
        else:
            b = (i - 2) // 2
            v_copy(b, b % SLOTS).start()

    q_copy.start()
    start(0)
    q_copy.wait()
    for i in range(1, FLIGHT):
        start(i)

    barrier = pltpu.get_barrier_semaphore()
    for step in range(1, n):
        pl.semaphore_signal(barrier, inc=1, device_id={"sp": lax.rem(me + step, n)}, device_id_type=MESH)

    def score(b, slot):
        return scores_of(q_ref[b], k_buf.at[slot]) * k_ref.shape[2] ** -0.5

    def soften(s):
        high = fold(jnp.max(s, 0, keepdims=True), jnp.maximum)
        p = jnp.exp(s - high)
        total = fold(jnp.sum(p, 0, keepdims=True), jnp.add)
        return p, jnp.where(lane[:1] < 64, high, total)

    def weigh(p, v):
        big = [jnp.where(diag, jnp.broadcast_to(p[r:r + 1], (8, 128)), 0.0) for r in range(p.shape[0])]
        return jnp.dot(jnp.concatenate(big, 1).astype(jnp.bfloat16), v, preferred_element_type=jnp.float32)

    steps = sorted(range(1, n), key=lambda step: -min(step, n - step))

    def part_copy(first, count, which, owner, step):
        block = gathered.at[owner, pl.ds(first, count)]
        return pltpu.make_async_remote_copy(block, block, send_sem.at[which, step], recv_sem.at[which, owner], device_id={"sp": lax.rem(me + step, n)}, device_id_type=MESH)

    def sum_copy(first, count, which, owner, step):
        block = sums.at[owner, pl.ds(first, count)]
        return pltpu.make_async_remote_copy(block, block, send_sum.at[which, step], recv_sum.at[which, owner], device_id={"sp": lax.rem(me + step, n)}, device_id_type=MESH)

    def send(copy, *which):
        for step in steps:
            copy(*which, me, step).start()

    def received(copy, *which):
        for step in steps:
            copy(*which, lax.rem(me + step, n), step).wait_recv()

    def sent(copy, *which):
        for step in steps:
            copy(*which, me, step).wait_send()

    def shares(b):
        rows = jnp.concatenate([sums[d, b] for d in range(n)], 0)
        high = jnp.max(rows, 0, keepdims=True)
        scale = jnp.exp(rows - high)
        total = jnp.sum(pltpu.roll(rows, 64, 1) * scale, 0, keepdims=True)
        scale = scale / total
        return [jnp.sum(jnp.where(lane == sub, jnp.broadcast_to(scale[d:d + 1], (8, 128)), 0.0), 1, keepdims=True) for d in range(n)]

    def combine(b, columns):
        result = [gathered[d, b].astype(jnp.float32) * columns[d] for d in range(n)]
        while len(result) > 1:
            result = [result[i] + result[i + 1] for i in range(0, len(result), 2)]
        o_ref[b] = result[0].astype(o_ref.dtype)

    main = batch - 2

    k_copy(0, 0).wait()
    start(FLIGHT)
    s0 = score(0, 0)
    k_copy(1, 1).wait()
    start(FLIGHT + 1)
    p0, row = soften(s0)
    s1 = score(1, 1)
    sums[me, 0] = row
    pl.semaphore_wait(barrier, n - 1)

    def body(b, carry):
        s, p = carry
        ahead = SLOTS - 1
        slot, k_slot = lax.rem(b, SLOTS), lax.rem(b + 2, SLOTS)
        v_copy(b, slot).wait()
        k_copy(b + 2, k_slot).wait()

        @pl.when(b + ahead < batch - 1)
        def _():
            v_copy(b + ahead, lax.rem(b + ahead, SLOTS)).start()

        @pl.when(b + ahead == batch - 1)
        def _():
            for piece in range(PIECES):
                last_copy(piece).start()

        @pl.when(b + 2 + ahead < batch)
        def _():
            k_copy(b + 2 + ahead, lax.rem(b + 2 + ahead, SLOTS)).start()

        gathered[me, b] = weigh(p, v_buf[slot]).astype(jnp.bfloat16)
        s_next = score(b + 2, k_slot)
        p_next, row = soften(s)
        sums[me, b + 1] = row

        @pl.when(lax.rem(b, GROUP) == GROUP - 1)
        def _():
            send(part_copy, b - (GROUP - 1), GROUP, 0)
            send(sum_copy, b - (GROUP - 1), GROUP, 0)

        return s_next, p_next

    s, p = lax.fori_loop(0, batch - 2, body, (s1, p0))
    last = batch - 1
    v_copy(main, main % SLOTS).wait()
    gathered[me, main] = weigh(p, v_buf[main % SLOTS]).astype(jnp.bfloat16)
    p, row = soften(s)
    sums[me, last] = row
    send(sum_copy, main, 2, 1)
    send(part_copy, main, 1, 1)
    rows, tokens = p.shape[0] // PIECES, v_buf.shape[1] // PIECES
    result = 0.0
    for piece in range(PIECES):
        last_copy(piece).wait()
        result += weigh(p[piece * rows:(piece + 1) * rows], v_buf[last % SLOTS, piece * tokens:(piece + 1) * tokens])
    gathered[me, last] = result.astype(jnp.bfloat16)
    send(part_copy, last, 1, 2)

    received(sum_copy, 0, main, 0)
    received(part_copy, 0, main, 0)

    def finish(i, _):
        columns = [shares(i * 5 + j) for j in range(5)]
        for j in range(5):
            combine(i * 5 + j, columns[j])
        return 0

    lax.fori_loop(0, main // 5, finish, 0)
    received(sum_copy, main, 2, 1)
    columns = [shares(main), shares(last)]
    received(part_copy, main, 1, 1)
    combine(main, columns[0])
    received(part_copy, last, 1, 2)
    combine(last, columns[1])
    sent(sum_copy, 0, main, 0)
    sent(part_copy, 0, main, 0)
    sent(sum_copy, main, 2, 1)
    sent(part_copy, main, 1, 1)
    sent(part_copy, last, 1, 2)


def solution(mesh):
    n = mesh.shape["sp"]

    def step(q, k, v):
        b, u, h, d = k.shape
        rows = u * h
        return pl.pallas_call(
            kernel,
            out_shape=jax.ShapeDtypeStruct((b, h, d), jnp.bfloat16),
            in_specs=[pl.BlockSpec(memory_space=pltpu.HBM)] * 3,
            out_specs=pl.BlockSpec(memory_space=pltpu.VMEM),
            scratch_shapes=[
                pltpu.VMEM((b, h, d), jnp.bfloat16),
                pltpu.VMEM((SLOTS, rows, d), jnp.bfloat16),
                pltpu.VMEM((SLOTS, rows, d), jnp.bfloat16),
                pltpu.VMEM((n, b, h, d), jnp.bfloat16),
                pltpu.VMEM((n, b, 1, 128), jnp.float32),
                pltpu.SemaphoreType.DMA,
                pltpu.SemaphoreType.DMA((SLOTS,)),
                pltpu.SemaphoreType.DMA((SLOTS,)),
                pltpu.SemaphoreType.DMA((PIECES,)),
                pltpu.SemaphoreType.DMA((3, n)),
                pltpu.SemaphoreType.DMA((3, n)),
                pltpu.SemaphoreType.DMA((3, n)),
                pltpu.SemaphoreType.DMA((3, n)),
            ],
            name="decode",
            compiler_params=pltpu.CompilerParams(collective_id=0, has_side_effects=True, vmem_limit_bytes=LIMIT << 20),
        )(pltpu.with_memory_space_constraint(q, pltpu.HBM), k.reshape(b, rows, d), v.reshape(b, rows, d))

    return jax.shard_map(
        step,
        mesh=mesh,
        in_specs=(P("dp", None, None), P("dp", "sp", None, None), P("dp", "sp", None, None)),
        out_specs=P("dp", None, None),
        check_vma=False,
    )
```

```python
import functools

import jax
import jax.numpy as jnp
from jax import lax
from jax.experimental import pallas as pl
from jax.experimental.pallas import tpu as pltpu
from jax.sharding import PartitionSpec as P

LEAD = 4
AHEAD = 3
SLOTS = AHEAD + 1
GROUP = 2
PIECES = 2
LIMIT = 32
MESH = pl.DeviceIdType.MESH


def iotas():
    return lax.broadcasted_iota(jnp.int32, (8, 128), 1), lax.broadcasted_iota(jnp.int32, (8, 128), 0)


def scores_of(q, k_ref):
    lane, sub = iotas()
    spread = jnp.concatenate([q] * 16, 0)
    full = lax.dot_general(k_ref[...], spread, (((1,), (1,)), ((), ())), preferred_element_type=jnp.float32)
    full = full.reshape(-1, 16, 8, 128)
    out = []
    for r in range(full.shape[0]):
        level = [full[r, i] for i in range(16)]
        bit = 8
        while len(level) > 1:
            level = [jnp.where((lane & bit) != 0, level[i + 1], level[i]) for i in range(0, len(level), 2)]
            bit *= 2
        out.append(jnp.sum(jnp.where((lane & 7) == sub, level[0], 0.0), 0, keepdims=True))
    return jnp.concatenate(out, 0)


def fold(x, op):
    turned = [x] + [pltpu.roll(x, s, 1) for s in range(8, 128, 8)]
    while len(turned) > 1:
        turned = [op(turned[i], turned[i + 1]) for i in range(0, len(turned), 2)]
    return turned[0]


def kernel(q_hbm, k_ref, v_ref, o_ref, q_ref, k_buf, v_buf, weights, gathered, sums, q_sem, k_sem, v_sem, send_sem, recv_sem, send_sum, recv_sum):
    batch = k_ref.shape[0]
    n = lax.axis_size("sp")
    me = lax.axis_index("sp")
    lane, sub = iotas()
    diag = (lane & 7) == sub

    last, main = batch - 1, batch - LEAD

    def k_copy(b):
        slot = lax.rem(b, SLOTS)
        return pltpu.make_async_copy(k_ref.at[b], k_buf.at[slot], k_sem.at[slot])

    tokens = v_ref.shape[1] // PIECES

    def v_copy(b, piece):
        slot, part = lax.rem(b, SLOTS), pl.ds(pl.multiple_of(piece * tokens, tokens), tokens)
        return pltpu.make_async_copy(v_ref.at[b, part], v_buf.at[slot, part], v_sem.at[slot, piece])

    def v_start(b):
        for piece in range(PIECES):
            v_copy(b, piece).start()

    q_copy = pltpu.make_async_copy(q_hbm, q_ref, q_sem)
    q_copy.start()
    k_copy(0).start()

    barrier = pltpu.get_barrier_semaphore()
    for step in range(1, n):
        pl.semaphore_signal(barrier, inc=1, device_id={"sp": lax.rem(me + step, n)}, device_id_type=MESH)

    def score(b):
        return scores_of(q_ref[b], k_buf.at[lax.rem(b, SLOTS)]) * k_ref.shape[2] ** -0.5

    def soften(b, s):
        high = fold(jnp.max(s, 0, keepdims=True), jnp.maximum)
        p = jnp.exp(s - high)
        total = fold(jnp.sum(p, 0, keepdims=True), jnp.add)
        weights[lax.rem(b, LEAD)] = p
        sums[me, b] = jnp.where(lane[:1] < 64, high, total)

    def weigh(p, v):
        big = [jnp.where(diag, jnp.broadcast_to(p[r:r + 1], (8, 128)), 0.0) for r in range(p.shape[0])]
        return jnp.dot(jnp.concatenate(big, 1).astype(jnp.bfloat16), v, preferred_element_type=jnp.float32)

    steps = sorted(range(1, n), key=lambda step: -min(step, n - step))

    def send(array, send_sem, recv_sem, first, count, which):
        block = array.at[me, pl.ds(first, count)]
        for step in steps:
            pltpu.make_async_remote_copy(block, block, send_sem.at[which], recv_sem.at[which], device_id={"sp": lax.rem(me + step, n)}, device_id_type=MESH).start()

    def everyone(array, send_sem, recv_sem, first, count, which):
        block = array.at[pl.ds(0, n - 1), pl.ds(first, count)]
        return pltpu.make_async_remote_copy(block, block, send_sem.at[which], recv_sem.at[which], device_id={"sp": lax.rem(me + 1, n)}, device_id_type=MESH)

    parts, part_sums = (gathered, send_sem, recv_sem), (sums, send_sum, recv_sum)

    def shares(b):
        rows = jnp.concatenate([sums[d, b] for d in range(n)], 0)
        high = jnp.max(rows, 0, keepdims=True)
        scale = jnp.exp(rows - high)
        total = jnp.sum(pltpu.roll(rows, 64, 1) * scale, 0, keepdims=True)
        scale = scale / total
        return [jnp.sum(jnp.where(lane == sub, jnp.broadcast_to(scale[d:d + 1], (8, 128)), 0.0), 1, keepdims=True) for d in range(n)]

    def combine(b, columns):
        result = [gathered[d, b].astype(jnp.float32) * columns[d] for d in range(n)]
        while len(result) > 1:
            result = [result[i] + result[i + 1] for i in range(0, len(result), 2)]
        o_ref[b] = result[0].astype(o_ref.dtype)

    q_copy.wait()
    for b in range(1, AHEAD):
        k_copy(b).start()

    def open_up(b, s):
        k_copy(b).wait()
        k_copy(b + AHEAD).start()

        @pl.when(b < AHEAD)
        def _():
            v_start(b)

        s_next = score(b)
        soften(jnp.maximum(b - 1, 0), s)
        return s_next

    s = lax.fori_loop(0, LEAD, open_up, jnp.zeros(weights.shape[1:], jnp.float32))
    pl.semaphore_wait(barrier, n - 1)

    def body(b, s):
        for piece in range(PIECES):
            v_copy(b, piece).wait()
        k_copy(b + LEAD).wait()
        v_start(b + AHEAD)

        @pl.when(b + LEAD + AHEAD < batch)
        def _():
            k_copy(b + LEAD + AHEAD).start()

        gathered[me, b] = weigh(weights[lax.rem(b, LEAD)], v_buf[lax.rem(b, SLOTS)]).astype(jnp.bfloat16)
        s_next = score(b + LEAD)
        soften(b + LEAD - 1, s)

        @pl.when(lax.rem(b, GROUP) == GROUP - 1)
        def _():
            send(*parts, b - (GROUP - 1), GROUP, 0)
            send(*part_sums, b - (GROUP - 1), GROUP, 0)

        return s_next

    s = lax.fori_loop(0, main, body, s)
    soften(last, s)
    send(*part_sums, main, LEAD, 1)

    def close_down(i, result):
        b, piece = main + i // PIECES, lax.rem(i, PIECES)
        v_copy(b, piece).wait()

        @pl.when((piece == 0) & (b + AHEAD < batch))
        def _():
            v_start(b + AHEAD)

        slot, rows = lax.rem(b, SLOTS), weights.shape[1] // PIECES
        p = weights[lax.rem(b, LEAD), pl.ds(pl.multiple_of(piece * rows, rows), rows)]
        v = v_buf[slot, pl.ds(pl.multiple_of(piece * tokens, tokens), tokens)]
        result = jnp.where(piece == 0, 0.0, result) + weigh(p, v)

        @pl.when(piece == PIECES - 1)
        def _():
            gathered[me, b] = result.astype(jnp.bfloat16)
            send(*parts, b, 1, 1 + i // PIECES)

        return result

    lax.fori_loop(0, LEAD * PIECES, close_down, jnp.zeros(o_ref.shape[1:], jnp.float32))

    everyone(*part_sums, 0, main, 0).wait_recv()
    everyone(*parts, 0, main, 0).wait_recv()

    def finish(i, _):
        columns = [shares(i * 4 + j) for j in range(4)]
        for j in range(4):
            combine(i * 4 + j, columns[j])
        return 0

    lax.fori_loop(0, main // 4, finish, 0)
    everyone(*part_sums, 0, main, 0).wait_send()
    everyone(*parts, 0, main, 0).wait_send()
    everyone(*part_sums, main, LEAD, 1).wait_send()
    everyone(*part_sums, main, LEAD, 1).wait_recv()

    def finish_last(i, _):
        columns = shares(main + i)
        everyone(*parts, main + i, 1, 1 + i).wait_send()
        everyone(*parts, main + i, 1, 1 + i).wait_recv()
        combine(main + i, columns)
        return 0

    lax.fori_loop(0, LEAD, finish_last, 0)


def solution(mesh):
    n = mesh.shape["sp"]

    def step(q, k, v):
        b, u, h, d = k.shape
        rows = u * h
        return pl.pallas_call(
            kernel,
            out_shape=jax.ShapeDtypeStruct((b, h, d), jnp.bfloat16),
            in_specs=[pl.BlockSpec(memory_space=pltpu.HBM)] * 3,
            out_specs=pl.BlockSpec(memory_space=pltpu.VMEM),
            scratch_shapes=[
                pltpu.VMEM((b, h, d), jnp.bfloat16),
                pltpu.VMEM((SLOTS, rows, d), jnp.bfloat16),
                pltpu.VMEM((SLOTS, rows, d), jnp.bfloat16),
                pltpu.VMEM((LEAD, rows // 128, 128), jnp.float32),
                pltpu.VMEM((n, b, h, d), jnp.bfloat16),
                pltpu.VMEM((n, b, 1, 128), jnp.float32),
                pltpu.SemaphoreType.DMA,
                pltpu.SemaphoreType.DMA((SLOTS,)),
                pltpu.SemaphoreType.DMA((SLOTS, PIECES)),
                pltpu.SemaphoreType.DMA((LEAD + 1,)),
                pltpu.SemaphoreType.DMA((LEAD + 1,)),
                pltpu.SemaphoreType.DMA((LEAD + 1,)),
                pltpu.SemaphoreType.DMA((LEAD + 1,)),
            ],
            name="decode",
            compiler_params=pltpu.CompilerParams(collective_id=0, has_side_effects=True, vmem_limit_bytes=LIMIT << 20),
        )(pltpu.with_memory_space_constraint(q, pltpu.HBM), k.reshape(b, rows, d), v.reshape(b, rows, d))

    return jax.shard_map(
        step,
        mesh=mesh,
        in_specs=(P("dp", None, None), P("dp", "sp", None, None), P("dp", "sp", None, None)),
        out_specs=P("dp", None, None),
        check_vma=False,
    )
```

```python
import functools

import jax
import jax.numpy as jnp
from jax import lax
from jax.experimental import pallas as pl
from jax.experimental.pallas import tpu as pltpu
from jax.sharding import PartitionSpec as P

LEAD = 4
AHEAD = 3
SLOTS = AHEAD + 1
GROUP = 2
PIECES = 1
LIMIT = 32
MESH = pl.DeviceIdType.MESH


def iotas():
    return lax.broadcasted_iota(jnp.int32, (8, 128), 1), lax.broadcasted_iota(jnp.int32, (8, 128), 0)


def scores_of(q, k_ref):
    lane, sub = iotas()
    spread = jnp.concatenate([q] * 16, 0)
    full = lax.dot_general(k_ref[...], spread, (((1,), (1,)), ((), ())), preferred_element_type=jnp.float32)
    full = full.reshape(-1, 16, 8, 128)
    out = []
    for r in range(full.shape[0]):
        level = [full[r, i] for i in range(16)]
        bit = 8
        while len(level) > 1:
            level = [jnp.where((lane & bit) != 0, level[i + 1], level[i]) for i in range(0, len(level), 2)]
            bit *= 2
        out.append(jnp.sum(jnp.where((lane & 7) == sub, level[0], 0.0), 0, keepdims=True))
    return jnp.concatenate(out, 0)


def fold(x, op):
    turned = [x] + [pltpu.roll(x, s, 1) for s in range(8, 128, 8)]
    while len(turned) > 1:
        turned = [op(turned[i], turned[i + 1]) for i in range(0, len(turned), 2)]
    return turned[0]


def kernel(q_hbm, k_ref, v_ref, o_ref, q_ref, k_buf, v_buf, weights, gathered, sums, q_sem, k_sem, v_sem, send_sem, recv_sem, send_sum, recv_sum):
    batch = k_ref.shape[0]
    n = lax.axis_size("sp")
    me = lax.axis_index("sp")
    lane, sub = iotas()
    diag = (lane & 7) == sub

    last, main = batch - 1, batch - LEAD

    def k_copy(b):
        slot = lax.rem(b, SLOTS)
        return pltpu.make_async_copy(k_ref.at[b], k_buf.at[slot], k_sem.at[slot])

    tokens = v_ref.shape[1] // PIECES

    def v_copy(b, piece):
        slot, part = lax.rem(b, SLOTS), pl.ds(pl.multiple_of(piece * tokens, tokens), tokens)
        return pltpu.make_async_copy(v_ref.at[b, part], v_buf.at[slot, part], v_sem.at[slot, piece])

    def v_start(b):
        for piece in range(PIECES):
            v_copy(b, piece).start()

    q_copy = pltpu.make_async_copy(q_hbm, q_ref, q_sem)
    q_copy.start()
    k_copy(0).start()

    barrier = pltpu.get_barrier_semaphore()
    for step in range(1, n):
        pl.semaphore_signal(barrier, inc=1, device_id={"sp": lax.rem(me + step, n)}, device_id_type=MESH)

    def score(b):
        return scores_of(q_ref[b], k_buf.at[lax.rem(b, SLOTS)]) * k_ref.shape[2] ** -0.5

    def soften(b, s):
        high = fold(jnp.max(s, 0, keepdims=True), jnp.maximum)
        p = jnp.exp(s - high)
        total = fold(jnp.sum(p, 0, keepdims=True), jnp.add)
        weights[lax.rem(b, LEAD)] = p
        sums[me, b] = jnp.where(lane[:1] < 64, high, total)

    def weigh(p, v):
        big = [jnp.where(diag, jnp.broadcast_to(p[r:r + 1], (8, 128)), 0.0) for r in range(p.shape[0])]
        return jnp.dot(jnp.concatenate(big, 1).astype(jnp.bfloat16), v, preferred_element_type=jnp.float32)

    steps = sorted(range(1, n), key=lambda step: -min(step, n - step))

    def send(array, send_sem, recv_sem, first, count, which):
        block = array.at[me, pl.ds(first, count)]
        for step in steps:
            pltpu.make_async_remote_copy(block, block, send_sem.at[which], recv_sem.at[which], device_id={"sp": lax.rem(me + step, n)}, device_id_type=MESH).start()

    def everyone(array, send_sem, recv_sem, first, count, which):
        block = array.at[pl.ds(0, n - 1), pl.ds(first, count)]
        return pltpu.make_async_remote_copy(block, block, send_sem.at[which], recv_sem.at[which], device_id={"sp": lax.rem(me + 1, n)}, device_id_type=MESH)

    parts, part_sums = (gathered, send_sem, recv_sem), (sums, send_sum, recv_sum)

    def shares(b):
        rows = jnp.concatenate([sums[d, b] for d in range(n)], 0)
        high = jnp.max(rows, 0, keepdims=True)
        scale = jnp.exp(rows - high)
        total = jnp.sum(pltpu.roll(rows, 64, 1) * scale, 0, keepdims=True)
        scale = scale / total
        return [jnp.sum(jnp.where(lane == sub, jnp.broadcast_to(scale[d:d + 1], (8, 128)), 0.0), 1, keepdims=True) for d in range(n)]

    def combine(b, columns):
        result = [gathered[d, b].astype(jnp.float32) * columns[d] for d in range(n)]
        while len(result) > 1:
            result = [result[i] + result[i + 1] for i in range(0, len(result), 2)]
        o_ref[b] = result[0].astype(o_ref.dtype)

    q_copy.wait()
    for b in range(1, AHEAD):
        k_copy(b).start()

    def open_up(b, s):
        k_copy(b).wait()
        k_copy(b + AHEAD).start()

        @pl.when(b < AHEAD)
        def _():
            v_start(b)

        s_next = score(b)
        soften(jnp.maximum(b - 1, 0), s)
        return s_next

    s = lax.fori_loop(0, LEAD, open_up, jnp.zeros(weights.shape[1:], jnp.float32))
    pl.semaphore_wait(barrier, n - 1)

    def body(b, s):
        for piece in range(PIECES):
            v_copy(b, piece).wait()
        k_copy(b + LEAD).wait()
        v_start(b + AHEAD)

        @pl.when(b + LEAD + AHEAD < batch)
        def _():
            k_copy(b + LEAD + AHEAD).start()

        gathered[me, b] = weigh(weights[lax.rem(b, LEAD)], v_buf[lax.rem(b, SLOTS)]).astype(jnp.bfloat16)
        s_next = score(b + LEAD)
        soften(b + LEAD - 1, s)

        @pl.when(lax.rem(b, GROUP) == GROUP - 1)
        def _():
            send(*parts, b - (GROUP - 1), GROUP, 0)
            send(*part_sums, b - (GROUP - 1), GROUP, 0)

        return s_next

    s = lax.fori_loop(0, main, body, s)
    v_start(last)
    soften(last, s)
    send(*part_sums, main, LEAD, 1)

    def close_down(i, result):
        b, piece = main + i // PIECES, lax.rem(i, PIECES)
        v_copy(b, piece).wait()

        slot, rows = lax.rem(b, SLOTS), weights.shape[1] // PIECES
        p = weights[lax.rem(b, LEAD), pl.ds(pl.multiple_of(piece * rows, rows), rows)]
        v = v_buf[slot, pl.ds(pl.multiple_of(piece * tokens, tokens), tokens)]
        result = jnp.where(piece == 0, 0.0, result) + weigh(p, v)

        @pl.when(piece == PIECES - 1)
        def _():
            gathered[me, b] = result.astype(jnp.bfloat16)
            send(*parts, b, 1, 1 + i // PIECES)

        return result

    lax.fori_loop(0, LEAD * PIECES, close_down, jnp.zeros(o_ref.shape[1:], jnp.float32))

    everyone(*part_sums, 0, main, 0).wait_recv()
    everyone(*parts, 0, main, 0).wait_recv()

    def finish(i, _):
        columns = [shares(i * 4 + j) for j in range(4)]
        for j in range(4):
            combine(i * 4 + j, columns[j])
        return 0

    lax.fori_loop(0, main // 4, finish, 0)
    everyone(*part_sums, 0, main, 0).wait_send()
    everyone(*parts, 0, main, 0).wait_send()
    everyone(*part_sums, main, LEAD, 1).wait_send()
    everyone(*part_sums, main, LEAD, 1).wait_recv()

    def finish_last(i, _):
        columns = shares(main + i)
        everyone(*parts, main + i, 1, 1 + i).wait_send()
        everyone(*parts, main + i, 1, 1 + i).wait_recv()
        combine(main + i, columns)
        return 0

    lax.fori_loop(0, LEAD, finish_last, 0)


def solution(mesh):
    n = mesh.shape["sp"]

    def step(q, k, v):
        b, u, h, d = k.shape
        rows = u * h
        return pl.pallas_call(
            kernel,
            out_shape=jax.ShapeDtypeStruct((b, h, d), jnp.bfloat16),
            in_specs=[pl.BlockSpec(memory_space=pltpu.HBM)] * 3,
            out_specs=pl.BlockSpec(memory_space=pltpu.VMEM),
            scratch_shapes=[
                pltpu.VMEM((b, h, d), jnp.bfloat16),
                pltpu.VMEM((SLOTS, rows, d), jnp.bfloat16),
                pltpu.VMEM((SLOTS, rows, d), jnp.bfloat16),
                pltpu.VMEM((LEAD, rows // 128, 128), jnp.float32),
                pltpu.VMEM((n, b, h, d), jnp.bfloat16),
                pltpu.VMEM((n, b, 1, 128), jnp.float32),
                pltpu.SemaphoreType.DMA,
                pltpu.SemaphoreType.DMA((SLOTS,)),
                pltpu.SemaphoreType.DMA((SLOTS, PIECES)),
                pltpu.SemaphoreType.DMA((LEAD + 1,)),
                pltpu.SemaphoreType.DMA((LEAD + 1,)),
                pltpu.SemaphoreType.DMA((LEAD + 1,)),
                pltpu.SemaphoreType.DMA((LEAD + 1,)),
            ],
            name="decode",
            compiler_params=pltpu.CompilerParams(collective_id=0, has_side_effects=True, vmem_limit_bytes=LIMIT << 20),
        )(pltpu.with_memory_space_constraint(q, pltpu.HBM), k.reshape(b, rows, d), v.reshape(b, rows, d))

    return jax.shard_map(
        step,
        mesh=mesh,
        in_specs=(P("dp", None, None), P("dp", "sp", None, None), P("dp", "sp", None, None)),
        out_specs=P("dp", None, None),
        check_vma=False,
    )
```

```python
import functools

import jax
import jax.numpy as jnp
from jax import lax
from jax.experimental import pallas as pl
from jax.experimental.pallas import tpu as pltpu
from jax.sharding import PartitionSpec as P

LEAD = 4
AHEAD = 3
SLOTS = AHEAD + 1
GROUP = 2
PIECES = 1
LIMIT = 32
MESH = pl.DeviceIdType.MESH


def iotas():
    return lax.broadcasted_iota(jnp.int32, (8, 128), 1), lax.broadcasted_iota(jnp.int32, (8, 128), 0)


def scores_of(q, k_ref):
    lane, sub = iotas()
    spread = jnp.concatenate([q] * 16, 0)
    full = lax.dot_general(k_ref[...], spread, (((1,), (1,)), ((), ())), preferred_element_type=jnp.float32)
    full = full.reshape(-1, 16, 8, 128)
    out = []
    for r in range(full.shape[0]):
        level = [full[r, i] for i in range(16)]
        bit = 8
        while len(level) > 1:
            level = [jnp.where((lane & bit) != 0, level[i + 1], level[i]) for i in range(0, len(level), 2)]
            bit *= 2
        out.append(jnp.sum(jnp.where((lane & 7) == sub, level[0], 0.0), 0, keepdims=True))
    return jnp.concatenate(out, 0)


def fold(x, op):
    turned = [x] + [pltpu.roll(x, s, 1) for s in range(8, 128, 8)]
    while len(turned) > 1:
        turned = [op(turned[i], turned[i + 1]) for i in range(0, len(turned), 2)]
    return turned[0]


def kernel(q_hbm, k_ref, v_ref, o_ref, q_ref, k_buf, v_buf, weights, gathered, sums, q_sem, k_sem, v_sem, send_sem, recv_sem, send_sum, recv_sum):
    batch = k_ref.shape[0]
    n = lax.axis_size("sp")
    me = lax.axis_index("sp")
    lane, sub = iotas()
    diag = (lane & 7) == sub

    last, main = batch - 1, batch - LEAD

    def k_copy(b):
        slot = lax.rem(b, SLOTS)
        return pltpu.make_async_copy(k_ref.at[b], k_buf.at[slot], k_sem.at[slot])

    tokens = v_ref.shape[1] // PIECES

    def v_copy(b, piece):
        slot, part = lax.rem(b, SLOTS), pl.ds(pl.multiple_of(piece * tokens, tokens), tokens)
        return pltpu.make_async_copy(v_ref.at[b, part], v_buf.at[slot, part], v_sem.at[slot, piece])

    def v_start(b):
        for piece in range(PIECES):
            v_copy(b, piece).start()

    q_copy = pltpu.make_async_copy(q_hbm, q_ref, q_sem)
    q_copy.start()
    k_copy(0).start()
    k_copy(1).start(priority=1)
    k_copy(2).start(priority=1)

    barrier = pltpu.get_barrier_semaphore()
    for step in range(1, n):
        pl.semaphore_signal(barrier, inc=1, device_id={"sp": lax.rem(me + step, n)}, device_id_type=MESH)

    def score(b):
        return scores_of(q_ref[b], k_buf.at[lax.rem(b, SLOTS)]) * k_ref.shape[2] ** -0.5

    def soften(b, s):
        high = fold(jnp.max(s, 0, keepdims=True), jnp.maximum)
        p = jnp.exp(s - high)
        total = fold(jnp.sum(p, 0, keepdims=True), jnp.add)
        weights[lax.rem(b, LEAD)] = p
        sums[me, b] = jnp.where(lane[:1] < 64, high, total)

    def weigh(p, v):
        big = [jnp.where(diag, jnp.broadcast_to(p[r:r + 1], (8, 128)), 0.0) for r in range(p.shape[0])]
        return jnp.dot(jnp.concatenate(big, 1).astype(jnp.bfloat16), v, preferred_element_type=jnp.float32)

    steps = sorted(range(1, n), key=lambda step: -min(step, n - step))

    def send(array, send_sem, recv_sem, first, count, which):
        block = array.at[me, pl.ds(first, count)]
        for step in steps:
            pltpu.make_async_remote_copy(block, block, send_sem.at[which], recv_sem.at[which], device_id={"sp": lax.rem(me + step, n)}, device_id_type=MESH).start()

    def everyone(array, send_sem, recv_sem, first, count, which):
        block = array.at[pl.ds(0, n - 1), pl.ds(first, count)]
        return pltpu.make_async_remote_copy(block, block, send_sem.at[which], recv_sem.at[which], device_id={"sp": lax.rem(me + 1, n)}, device_id_type=MESH)

    parts, part_sums = (gathered, send_sem, recv_sem), (sums, send_sum, recv_sum)

    def shares(b):
        rows = jnp.concatenate([sums[d, b] for d in range(n)], 0)
        high = jnp.max(rows, 0, keepdims=True)
        scale = jnp.exp(rows - high)
        total = jnp.sum(pltpu.roll(rows, 64, 1) * scale, 0, keepdims=True)
        scale = scale / total
        return [jnp.sum(jnp.where(lane == sub, jnp.broadcast_to(scale[d:d + 1], (8, 128)), 0.0), 1, keepdims=True) for d in range(n)]

    def combine(b, columns):
        result = [gathered[d, b].astype(jnp.float32) * columns[d] for d in range(n)]
        while len(result) > 1:
            result = [result[i] + result[i + 1] for i in range(0, len(result), 2)]
        o_ref[b] = result[0].astype(o_ref.dtype)

    q_copy.wait()

    def open_up(b, s):
        k_copy(b).wait()
        k_copy(b + AHEAD).start()

        @pl.when(b < AHEAD)
        def _():
            v_start(b)

        s_next = score(b)
        soften(jnp.maximum(b - 1, 0), s)
        return s_next

    s = lax.fori_loop(0, LEAD, open_up, jnp.zeros(weights.shape[1:], jnp.float32))
    pl.semaphore_wait(barrier, n - 1)

    def body(b, s):
        for piece in range(PIECES):
            v_copy(b, piece).wait()
        k_copy(b + LEAD).wait()
        v_start(b + AHEAD)

        @pl.when(b + LEAD + AHEAD < batch)
        def _():
            k_copy(b + LEAD + AHEAD).start()

        gathered[me, b] = weigh(weights[lax.rem(b, LEAD)], v_buf[lax.rem(b, SLOTS)]).astype(jnp.bfloat16)
        s_next = score(b + LEAD)
        soften(b + LEAD - 1, s)

        @pl.when(lax.rem(b, GROUP) == GROUP - 1)
        def _():
            send(*parts, b - (GROUP - 1), GROUP, 0)
            send(*part_sums, b - (GROUP - 1), GROUP, 0)

        return s_next

    s = lax.fori_loop(0, main, body, s)
    v_start(last)
    soften(last, s)
    send(*part_sums, main, LEAD, 1)

    def close_down(i, result):
        b, piece = main + i // PIECES, lax.rem(i, PIECES)
        v_copy(b, piece).wait()

        slot, rows = lax.rem(b, SLOTS), weights.shape[1] // PIECES
        p = weights[lax.rem(b, LEAD), pl.ds(pl.multiple_of(piece * rows, rows), rows)]
        v = v_buf[slot, pl.ds(pl.multiple_of(piece * tokens, tokens), tokens)]
        result = jnp.where(piece == 0, 0.0, result) + weigh(p, v)

        @pl.when(piece == PIECES - 1)
        def _():
            gathered[me, b] = result.astype(jnp.bfloat16)
            send(*parts, b, 1, 1 + i // PIECES)

        return result

    lax.fori_loop(0, LEAD * PIECES, close_down, jnp.zeros(o_ref.shape[1:], jnp.float32))

    everyone(*part_sums, 0, main, 0).wait_recv()
    everyone(*parts, 0, main, 0).wait_recv()

    def finish(i, _):
        columns = [shares(i * 4 + j) for j in range(4)]
        for j in range(4):
            combine(i * 4 + j, columns[j])
        return 0

    lax.fori_loop(0, main // 4, finish, 0)
    everyone(*part_sums, 0, main, 0).wait_send()
    everyone(*parts, 0, main, 0).wait_send()
    everyone(*part_sums, main, LEAD, 1).wait_send()
    everyone(*part_sums, main, LEAD, 1).wait_recv()

    def finish_last(i, _):
        columns = shares(main + i)
        everyone(*parts, main + i, 1, 1 + i).wait_send()
        everyone(*parts, main + i, 1, 1 + i).wait_recv()
        combine(main + i, columns)
        return 0

    lax.fori_loop(0, LEAD, finish_last, 0)


def solution(mesh):
    n = mesh.shape["sp"]

    def step(q, k, v):
        b, u, h, d = k.shape
        rows = u * h
        return pl.pallas_call(
            kernel,
            out_shape=jax.ShapeDtypeStruct((b, h, d), jnp.bfloat16),
            in_specs=[pl.BlockSpec(memory_space=pltpu.HBM)] * 3,
            out_specs=pl.BlockSpec(memory_space=pltpu.VMEM),
            scratch_shapes=[
                pltpu.VMEM((b, h, d), jnp.bfloat16),
                pltpu.VMEM((SLOTS, rows, d), jnp.bfloat16),
                pltpu.VMEM((SLOTS, rows, d), jnp.bfloat16),
                pltpu.VMEM((LEAD, rows // 128, 128), jnp.float32),
                pltpu.VMEM((n, b, h, d), jnp.bfloat16),
                pltpu.VMEM((n, b, 1, 128), jnp.float32),
                pltpu.SemaphoreType.DMA,
                pltpu.SemaphoreType.DMA((SLOTS,)),
                pltpu.SemaphoreType.DMA((SLOTS, PIECES)),
                pltpu.SemaphoreType.DMA((LEAD + 1,)),
                pltpu.SemaphoreType.DMA((LEAD + 1,)),
                pltpu.SemaphoreType.DMA((LEAD + 1,)),
                pltpu.SemaphoreType.DMA((LEAD + 1,)),
            ],
            name="decode",
            compiler_params=pltpu.CompilerParams(collective_id=0, has_side_effects=True, vmem_limit_bytes=LIMIT << 20),
        )(pltpu.with_memory_space_constraint(q, pltpu.HBM), k.reshape(b, rows, d), v.reshape(b, rows, d))

    return jax.shard_map(
        step,
        mesh=mesh,
        in_specs=(P("dp", None, None), P("dp", "sp", None, None), P("dp", "sp", None, None)),
        out_specs=P("dp", None, None),
        check_vma=False,
    )
```

```python
import functools

import jax
import jax.numpy as jnp
from jax import lax
from jax.experimental import pallas as pl
from jax.experimental.pallas import tpu as pltpu
from jax.sharding import PartitionSpec as P

LEAD = 4
AHEAD = 3
SLOTS = AHEAD + 1
GROUP = 2
SUMS = 8
PIECES = 1
LIMIT = 32
MESH = pl.DeviceIdType.MESH


def iotas():
    return lax.broadcasted_iota(jnp.int32, (8, 128), 1), lax.broadcasted_iota(jnp.int32, (8, 128), 0)


def scores_of(q, k_ref):
    lane, sub = iotas()
    spread = jnp.concatenate([q] * 16, 0)
    full = lax.dot_general(k_ref[...], spread, (((1,), (1,)), ((), ())), preferred_element_type=jnp.float32)
    full = full.reshape(-1, 16, 8, 128)
    out = []
    for r in range(full.shape[0]):
        level = [full[r, i] for i in range(16)]
        bit = 8
        while len(level) > 1:
            level = [jnp.where((lane & bit) != 0, level[i + 1], level[i]) for i in range(0, len(level), 2)]
            bit *= 2
        out.append(jnp.sum(jnp.where((lane & 7) == sub, level[0], 0.0), 0, keepdims=True))
    return jnp.concatenate(out, 0)


def fold(x, op):
    turned = [x] + [pltpu.roll(x, s, 1) for s in range(8, 128, 8)]
    while len(turned) > 1:
        turned = [op(turned[i], turned[i + 1]) for i in range(0, len(turned), 2)]
    return turned[0]


def kernel(q_hbm, k_ref, v_ref, o_ref, q_ref, k_buf, v_buf, weights, gathered, sums, q_sem, k_sem, v_sem, send_sem, recv_sem, send_sum, recv_sum):
    batch = k_ref.shape[0]
    n = lax.axis_size("sp")
    me = lax.axis_index("sp")
    lane, sub = iotas()
    diag = (lane & 7) == sub

    last, main = batch - 1, batch - LEAD

    def k_copy(b):
        slot = lax.rem(b, SLOTS)
        return pltpu.make_async_copy(k_ref.at[b], k_buf.at[slot], k_sem.at[slot])

    tokens = v_ref.shape[1] // PIECES

    def v_copy(b, piece):
        slot, part = lax.rem(b, SLOTS), pl.ds(pl.multiple_of(piece * tokens, tokens), tokens)
        return pltpu.make_async_copy(v_ref.at[b, part], v_buf.at[slot, part], v_sem.at[slot, piece])

    def v_start(b):
        for piece in range(PIECES):
            v_copy(b, piece).start()

    q_copy = pltpu.make_async_copy(q_hbm, q_ref, q_sem)
    q_copy.start()
    k_copy(0).start()
    k_copy(1).start(priority=1)
    k_copy(2).start(priority=1)

    barrier = pltpu.get_barrier_semaphore()
    for step in range(1, n):
        pl.semaphore_signal(barrier, inc=1, device_id={"sp": lax.rem(me + step, n)}, device_id_type=MESH)

    def score(b):
        return scores_of(q_ref[b], k_buf.at[lax.rem(b, SLOTS)]) * k_ref.shape[2] ** -0.5

    def soften(b, s):
        high = fold(jnp.max(s, 0, keepdims=True), jnp.maximum)
        p = jnp.exp(s - high)
        total = fold(jnp.sum(p, 0, keepdims=True), jnp.add)
        weights[lax.rem(b, LEAD)] = p
        sums[me, b] = jnp.where(lane[:1] < 64, high, total)

    def weigh(p, v):
        big = [jnp.where(diag, jnp.broadcast_to(p[r:r + 1], (8, 128)), 0.0) for r in range(p.shape[0])]
        return jnp.dot(jnp.concatenate(big, 1).astype(jnp.bfloat16), v, preferred_element_type=jnp.float32)

    steps = sorted(range(1, n), key=lambda step: -min(step, n - step))

    def send(array, send_sem, recv_sem, first, count, which):
        block = array.at[me, pl.ds(first, count)]
        for step in steps:
            pltpu.make_async_remote_copy(block, block, send_sem.at[which], recv_sem.at[which], device_id={"sp": lax.rem(me + step, n)}, device_id_type=MESH).start()

    def everyone(array, send_sem, recv_sem, first, count, which):
        block = array.at[pl.ds(0, n - 1), pl.ds(first, count)]
        return pltpu.make_async_remote_copy(block, block, send_sem.at[which], recv_sem.at[which], device_id={"sp": lax.rem(me + 1, n)}, device_id_type=MESH)

    parts, part_sums = (gathered, send_sem, recv_sem), (sums, send_sum, recv_sum)

    def shares(b):
        rows = jnp.concatenate([sums[d, b] for d in range(n)], 0)
        high = jnp.max(rows, 0, keepdims=True)
        scale = jnp.exp(rows - high)
        total = jnp.sum(pltpu.roll(rows, 64, 1) * scale, 0, keepdims=True)
        scale = scale / total
        return [jnp.sum(jnp.where(lane == sub, jnp.broadcast_to(scale[d:d + 1], (8, 128)), 0.0), 1, keepdims=True) for d in range(n)]

    def combine(b, columns):
        result = [gathered[d, b].astype(jnp.float32) * columns[d] for d in range(n)]
        while len(result) > 1:
            result = [result[i] + result[i + 1] for i in range(0, len(result), 2)]
        o_ref[b] = result[0].astype(o_ref.dtype)

    q_copy.wait()

    def open_up(b, s):
        k_copy(b).wait()
        k_copy(b + AHEAD).start()

        @pl.when(b < AHEAD)
        def _():
            v_start(b)

        s_next = score(b)
        soften(jnp.maximum(b - 1, 0), s)
        return s_next

    s = lax.fori_loop(0, LEAD, open_up, jnp.zeros(weights.shape[1:], jnp.float32))
    pl.semaphore_wait(barrier, n - 1)

    def body(b, s):
        for piece in range(PIECES):
            v_copy(b, piece).wait()
        k_copy(b + LEAD).wait()
        v_start(b + AHEAD)

        @pl.when(b + LEAD + AHEAD < batch)
        def _():
            k_copy(b + LEAD + AHEAD).start()

        gathered[me, b] = weigh(weights[lax.rem(b, LEAD)], v_buf[lax.rem(b, SLOTS)]).astype(jnp.bfloat16)
        s_next = score(b + LEAD)
        soften(b + LEAD - 1, s)

        @pl.when(lax.rem(b, GROUP) == GROUP - 1)
        def _():
            send(*parts, b - (GROUP - 1), GROUP, 0)

        @pl.when(lax.rem(b, SUMS) == SUMS - 1)
        def _():
            send(*part_sums, b - (SUMS - 1), SUMS, 0)

        return s_next

    s = lax.fori_loop(0, main, body, s)
    v_start(last)
    soften(last, s)
    send(*part_sums, batch - SUMS, SUMS, 1)

    def close_down(i, result):
        b, piece = main + i // PIECES, lax.rem(i, PIECES)
        v_copy(b, piece).wait()

        slot, rows = lax.rem(b, SLOTS), weights.shape[1] // PIECES
        p = weights[lax.rem(b, LEAD), pl.ds(pl.multiple_of(piece * rows, rows), rows)]
        v = v_buf[slot, pl.ds(pl.multiple_of(piece * tokens, tokens), tokens)]
        result = jnp.where(piece == 0, 0.0, result) + weigh(p, v)

        @pl.when(piece == PIECES - 1)
        def _():
            gathered[me, b] = result.astype(jnp.bfloat16)
            send(*parts, b, 1, 1 + i // PIECES)

        return result

    lax.fori_loop(0, LEAD * PIECES, close_down, jnp.zeros(o_ref.shape[1:], jnp.float32))

    everyone(*part_sums, 0, batch - SUMS, 0).wait_recv()
    everyone(*parts, 0, main, 0).wait_recv()

    def finish(i, _):
        @pl.when(i == (batch - SUMS) // 4)
        def _():
            everyone(*part_sums, batch - SUMS, SUMS, 1).wait_recv()

        columns = [shares(i * 4 + j) for j in range(4)]
        for j in range(4):
            combine(i * 4 + j, columns[j])
        return 0

    lax.fori_loop(0, main // 4, finish, 0)
    everyone(*part_sums, 0, batch - SUMS, 0).wait_send()
    everyone(*parts, 0, main, 0).wait_send()
    everyone(*part_sums, batch - SUMS, SUMS, 1).wait_send()

    def finish_last(i, _):
        columns = shares(main + i)
        everyone(*parts, main + i, 1, 1 + i).wait_send()
        everyone(*parts, main + i, 1, 1 + i).wait_recv()
        combine(main + i, columns)
        return 0

    lax.fori_loop(0, LEAD, finish_last, 0)


def solution(mesh):
    n = mesh.shape["sp"]

    def step(q, k, v):
        b, u, h, d = k.shape
        rows = u * h
        return pl.pallas_call(
            kernel,
            out_shape=jax.ShapeDtypeStruct((b, h, d), jnp.bfloat16),
            in_specs=[pl.BlockSpec(memory_space=pltpu.HBM)] * 3,
            out_specs=pl.BlockSpec(memory_space=pltpu.VMEM),
            scratch_shapes=[
                pltpu.VMEM((b, h, d), jnp.bfloat16),
                pltpu.VMEM((SLOTS, rows, d), jnp.bfloat16),
                pltpu.VMEM((SLOTS, rows, d), jnp.bfloat16),
                pltpu.VMEM((LEAD, rows // 128, 128), jnp.float32),
                pltpu.VMEM((n, b, h, d), jnp.bfloat16),
                pltpu.VMEM((n, b, 1, 128), jnp.float32),
                pltpu.SemaphoreType.DMA,
                pltpu.SemaphoreType.DMA((SLOTS,)),
                pltpu.SemaphoreType.DMA((SLOTS, PIECES)),
                pltpu.SemaphoreType.DMA((LEAD + 1,)),
                pltpu.SemaphoreType.DMA((LEAD + 1,)),
                pltpu.SemaphoreType.DMA((LEAD + 1,)),
                pltpu.SemaphoreType.DMA((LEAD + 1,)),
            ],
            name="decode",
            compiler_params=pltpu.CompilerParams(collective_id=0, has_side_effects=True, vmem_limit_bytes=LIMIT << 20),
        )(pltpu.with_memory_space_constraint(q, pltpu.HBM), k.reshape(b, rows, d), v.reshape(b, rows, d))

    return jax.shard_map(
        step,
        mesh=mesh,
        in_specs=(P("dp", None, None), P("dp", "sp", None, None), P("dp", "sp", None, None)),
        out_specs=P("dp", None, None),
        check_vma=False,
    )
```
